32 devices in a mesh: seq: 4 (over y, x), exp: 8 (over z, core).
Axes of the slice: x: 2, y: 2, z: 4, core: 2. Of those that a mesh axis runs over, the one named last changes fastest.
Arguments:
- queries: bfloat16 [4096, 3072], P(('seq', 'exp')), may hold values from -123 to 123
- keys: bfloat16 [4096, 512], P(('seq', 'exp')), may hold values from -6 to 6
- values: bfloat16 [4096, 512], P(('seq', 'exp')), may hold values from -9 to 9
- residual: bfloat16 [4096, 6144], P(('seq', 'exp')), may hold values from -51 to 51
- proj_weight: bfloat16 [3072, 6144], P('seq', 'exp'), may hold values from -0.109375 to 0.109375
- norm_gain: bfloat16 [6144], replicated, may hold values from 0.099609375 to 1.8984375
- router: bfloat16 [6144, 8], replicated, may hold values from -0.078125 to 0.078125
- expert_ids: int32 [4096, 2], P(('seq', 'exp')), may hold values from 0 to 7, all different within a row; in each aligned block of 128 rows (0 to 127, 128 to 255, ...) at most 33 rows name the same one
- u_gate_up: bfloat16 [8, 6144, 1024], P('exp'), may hold values from -0.078125 to 0.078125
- v_gate_up: bfloat16 [8, 2, 512, 8192], P('exp'), may hold values from -0.25 to 0.25
- u_down: bfloat16 [8, 8192, 512], P('exp'), may hold values from -0.0625 to 0.0625
- v_down: bfloat16 [8, 512, 6144], P('exp'), may hold values from -0.25 to 0.25
Outputs:
- layer_out: bfloat16 [4096, 6144], P(('seq', 'exp'))
The draws below stay inside these ranges and needn't reach their ends.
Inputs may be any that keep to these rules, and one draw needn't show every extreme that they name: `expert_ids`: the two experts of a token differ. Among the tokens of one device no expert is named more than 33 times, and in some devices' tokens some expert is named exactly 33 times.
All inputs are finite; a program needn't handle non-finite values.
Results may differ from the reference program's by a relative error of at most 0.02.
Values may be sent and summed in bfloat16 or wider, within the bound.
A program may use at most 192 MiB of HBM per device.

```python
import math
import jax
import jax.numpy as jnp
import numpy as np
from jax import lax

D = 6144
HEADS = 24
KV_HEADS = 4
HEAD_DIM = 128
EXPERTS = 8
TOP = 2
RANK = 512
FF = 8192
TOK_DEV = 128
CAP = 33
PIECES = 1
TOKENS = 4096


def draw_queries(key, part):
    noise_draw = jax.random.normal(jax.random.fold_in(key, 902), (TOKENS, HEADS, HEAD_DIM), jnp.float32)
    noise_draw = jnp.clip(noise_draw, -6.0, 6.0)
    return noise_draw.reshape(TOKENS, HEADS * HEAD_DIM).astype(jnp.bfloat16)


def draw_keys(key, part):
    noise_draw = jax.random.normal(jax.random.fold_in(key, 903), (TOKENS, KV_HEADS, HEAD_DIM), jnp.float32)
    noise_draw = jnp.clip(noise_draw, -6.0, 6.0)
    return noise_draw.reshape(TOKENS, KV_HEADS * HEAD_DIM).astype(jnp.bfloat16)


def draw_values(key, part):
    noise_draw = jax.random.normal(jax.random.fold_in(key, 904), (TOKENS, KV_HEADS * HEAD_DIM), jnp.float32)
    noise_draw = jnp.clip(noise_draw, -6.0, 6.0)
    levels = jax.random.normal(jax.random.fold_in(key, 905), (TOKENS // 256, KV_HEADS * HEAD_DIM), jnp.float32)
    levels = jnp.clip(levels, -3.0, 3.0)
    level_rows = jnp.repeat(levels, 256, axis=0)
    return (noise_draw + level_rows).astype(jnp.bfloat16)


def draw_residual(key, part):
    noise_draw = jax.random.normal(jax.random.fold_in(key, 907), (TOKENS, D), jnp.float32)
    noise_draw = jnp.clip(noise_draw, -4.0, 4.0)
    return noise_draw.astype(jnp.bfloat16)


def block_levels(own_key, dims, shards, least, top_value):
    gain = 1.0
    for dim, parts in shards:
        heights = jax.random.uniform(jax.random.fold_in(jax.random.fold_in(own_key, 6), dim), (parts,), jnp.float32, least / len(shards), top_value / len(shards))
        gain = gain * jnp.repeat(jnp.exp(heights), dims[dim] // parts).reshape((-1,) + (1,) * (len(dims) - 1 - dim))
    return gain


def assign_block(own_key, own, number, rows, number_of, top, limit, slope):
    ranking = jax.random.permutation(own_key, number_of)
    heavy_load, ordinary = load_shares(number_of, rows * top, limit, slope, True), load_shares(number_of, rows * top, limit, slope, False)
    places = jnp.arange(number_of)

    def named(lengths, turn):
        used = int((lengths > 0).sum())
        fixed = max(1, used // 4)
        passed = fixed + (places - fixed + turn * (used - fixed)) % max(1, number_of - fixed)
        return jnp.zeros((number_of,), jnp.int32).at[ranking[jnp.where(places < fixed, places, passed)]].set(jnp.asarray(lengths, jnp.int32))

    lengths = jnp.where(number % 4 == 0, named(heavy_load, number // 4), named(ordinary, number - number // 4 - 1))
    mixed = jax.random.permutation(jax.random.fold_in(own, 3), number_of)
    giver, sink = mixed[0:number_of // 2 * 2:2], mixed[1:number_of // 2 * 2:2]
    slack = jnp.minimum(lengths[giver] - 1, limit - lengths[sink]) // 2
    slack = jnp.where((giver == ranking[0]) | (sink == ranking[0]) | (lengths[sink] == 0), 0, jnp.maximum(slack, 0))
    passed = jax.random.randint(jax.random.fold_in(own, 4), (number_of // 2,), 0, 1 << 20) % (slack + 1)
    lengths = lengths.at[giver].add(-passed).at[sink].add(passed)
    items = jnp.searchsorted(jnp.cumsum(lengths), jnp.arange(rows * top), side="right").astype(jnp.int32)
    grid = items.reshape(top, rows).T
    grid = grid[jax.random.permutation(jax.random.fold_in(own, 1), rows)]
    turn = jax.random.randint(jax.random.fold_in(own, 2), (rows, 1), 0, top)
    return jnp.take_along_axis(grid, (jnp.arange(top)[None, :] + turn) % top, axis=1)


def load_shares(amount, total, most, slope, full):
    weights = [(1 << 20) // math.isqrt(rank ** slope) + 1 for rank in range(1, amount + 1)]
    largest = most if full else min(most, max(-(-total // amount), total * weights[0] // sum(weights)))
    least = 1 if total - largest >= amount - 1 else 0
    given, surplus = [largest] + [least] * (amount - 1), total - largest - least * (amount - 1)
    while surplus > 0:
        movable = [i for i in range(1, amount) if given[i] < largest] or [i for i in range(1, amount) if given[i] < most]
        whole, left = sum([weights[i] for i in movable]), surplus
        for i in movable:
            more = min(most - given[i], max(1, left * weights[i] // whole), surplus)
            given[i] = given[i] + more
            surplus = surplus - more
    return np.array(given)


def normal_values(key, shape, scale, bound, split=(), kind=jnp.bfloat16):
    factor_of = block_levels(key, shape, split, -0.22, 0.18) if split else 1.0
    drawn = jax.random.normal(key, shape, jnp.float32) * scale * factor_of
    return jnp.minimum(jnp.maximum(drawn, -bound), bound).astype(kind)


def setup_inputs(seed: int = 0) -> dict:
    streams_of = jax.random.split(jax.random.key(seed), 13)
    queries = draw_queries(jax.random.fold_in(streams_of[12], 71), 0)
    keys = draw_keys(jax.random.fold_in(streams_of[12], 71), 0)
    values = draw_values(jax.random.fold_in(streams_of[12], 71), 0)
    residual = draw_residual(jax.random.fold_in(streams_of[12], 71), 0)
    proj_weight = normal_values(streams_of[4], (HEADS * HEAD_DIM, D), (HEADS * HEAD_DIM) ** -0.5, 0.109375, ((0, 4), (1, 8)))
    norm_gain = jnp.clip(1.0 + 0.18 * jax.random.normal(streams_of[5], (D,), jnp.float32), 0.099609375, 1.8984375).astype(jnp.bfloat16)
    router = normal_values(streams_of[6], (D, EXPERTS), D ** -0.5, 0.078125)
    expert_ids_keys = jax.random.split(jax.random.fold_in(streams_of[7], 1), TOKENS // TOK_DEV)
    expert_ids_turns = jax.random.permutation(jax.random.fold_in(streams_of[7], 3), TOKENS // TOK_DEV)
    expert_ids = jax.vmap(lambda own, number: assign_block(jax.random.fold_in(streams_of[7], 2), own, number, TOK_DEV, EXPERTS, TOP, CAP, 2))(expert_ids_keys, expert_ids_turns).reshape((TOKENS, TOP))
    u_gate_up = normal_values(streams_of[8], (EXPERTS * PIECES, D // PIECES, 2 * RANK), D ** -0.5, 0.078125, ((0, 8),))
    v_gate_up = normal_values(streams_of[9], (EXPERTS * PIECES, 2, RANK, FF // PIECES), RANK ** -0.5, 0.25, ((0, 8),))
    u_down = normal_values(streams_of[10], (EXPERTS * PIECES, FF // PIECES, RANK), FF ** -0.5, 0.0625, ((0, 8),))
    v_down = normal_values(streams_of[11], (EXPERTS * PIECES, RANK, D // PIECES), RANK ** -0.5, 0.25, ((0, 8),))
    return {"queries": queries, "keys": keys, "values": values, "residual": residual, "proj_weight": proj_weight, "norm_gain": norm_gain, "router": router, "expert_ids": expert_ids, "u_gate_up": u_gate_up, "v_gate_up": v_gate_up, "u_down": u_down, "v_down": v_down}


EPS = 1e-05

def causal_attention(queries, keys, values):
    tile_rows = min(1024, TOKENS)
    tile_count = TOKENS // tile_rows
    per_kv = HEADS // KV_HEADS
    query_tiles = queries.reshape(tile_count, tile_rows, KV_HEADS, per_kv, HEAD_DIM)
    key_tiles = keys.reshape(tile_count, tile_rows, KV_HEADS, HEAD_DIM)
    value_tiles = values.reshape(tile_count, tile_rows, KV_HEADS, HEAD_DIM)
    score_scale = HEAD_DIM ** (-0.5)
    offsets = jnp.arange(tile_rows, dtype=jnp.int32)

    def one_tile(tile_index):
        query_block = lax.dynamic_index_in_dim(query_tiles, tile_index, 0, keepdims=False).astype(jnp.float32)
        query_pos = tile_index * tile_rows + offsets

        def scores_of(key_index):
            key_block = lax.dynamic_index_in_dim(key_tiles, key_index, 0, keepdims=False).astype(jnp.float32)
            scores = jnp.einsum('qhjd,khd->hjqk', query_block, key_block) * score_scale
            key_pos = key_index * tile_rows + offsets
            allowed = key_pos[None, :] <= query_pos[:, None]
            return jnp.where(allowed[None, None], scores, -jnp.inf)

        def max_step(key_index, row_max):
            return jnp.maximum(row_max, lax.optimization_barrier(jnp.max(scores_of(key_index), axis=-1)))
        start_max = jnp.full((KV_HEADS, per_kv, tile_rows), -jnp.inf, jnp.float32)
        row_max = lax.fori_loop(jnp.int32(0), tile_index + 1, max_step, start_max)

        def sum_step(key_index, carried):
            row_sum, weighted = carried
            exp_terms = jnp.exp(scores_of(key_index) - row_max[..., None])
            rounded = lax.optimization_barrier(exp_terms.astype(jnp.bfloat16)).astype(jnp.float32)
            value_block = lax.dynamic_index_in_dim(value_tiles, key_index, 0, keepdims=False).astype(jnp.float32)
            row_sum = row_sum + lax.optimization_barrier(jnp.sum(exp_terms, axis=-1))
            weighted = weighted + jnp.einsum('hjqk,khd->hjqd', rounded, value_block)
            return (row_sum, weighted)
        start_sum = jnp.zeros((KV_HEADS, per_kv, tile_rows), jnp.float32)
        start_acc = jnp.zeros((KV_HEADS, per_kv, tile_rows, HEAD_DIM), jnp.float32)
        row_sum, weighted = lax.fori_loop(jnp.int32(0), tile_index + 1, sum_step, (start_sum, start_acc))
        result = weighted / row_sum[..., None]
        return jnp.transpose(result, (2, 0, 1, 3)).reshape(tile_rows, HEADS * HEAD_DIM)
    outputs = lax.map(one_tile, jnp.arange(tile_count, dtype=jnp.int32))
    return outputs.reshape(TOKENS, HEADS * HEAD_DIM).astype(jnp.bfloat16)

def expert_stack(u_gate_up, v_gate_up, u_down, v_down):
    first_in = u_gate_up.reshape(EXPERTS, D, 2 * RANK)
    second_in = jnp.transpose(v_gate_up.reshape(EXPERTS, PIECES, 2, RANK, FF // PIECES), (0, 2, 3, 1, 4))
    second_in = second_in.reshape(EXPERTS, 2, RANK, FF)
    first_out = u_down.reshape(EXPERTS, FF, RANK)
    second_out = jnp.transpose(v_down.reshape(EXPERTS, PIECES, RANK, D // PIECES), (0, 2, 1, 3))
    second_out = second_out.reshape(EXPERTS, RANK, D)
    return (first_in, second_in, first_out, second_out)

def reference(queries, keys, values, residual, proj_weight, norm_gain, router, expert_ids, u_gate_up, v_gate_up, u_down, v_down):
    attended = causal_attention(queries, keys, values)
    attn_update = jnp.dot(attended, proj_weight, preferred_element_type=jnp.float32).astype(jnp.bfloat16)
    stream = residual.astype(jnp.float32) + attn_update.astype(jnp.float32)
    mean_sq = lax.optimization_barrier(jnp.mean(stream * stream, axis=-1, keepdims=True))
    normed = (stream * lax.rsqrt(mean_sq + EPS) * norm_gain.astype(jnp.float32)).astype(jnp.bfloat16)
    logits = jnp.dot(normed, router, preferred_element_type=jnp.float32)
    expert_range = jnp.arange(EXPERTS, dtype=jnp.int32)
    picked = (expert_ids[:, :, None] == expert_range[None, None, :]).astype(jnp.float32)
    chosen = lax.optimization_barrier(jnp.sum(picked * logits[:, None, :], axis=-1))
    mix_first = jax.nn.sigmoid(chosen[:, 0] - chosen[:, 1])
    mix_second = jax.nn.sigmoid(chosen[:, 1] - chosen[:, 0])
    mix_weight = jnp.stack([mix_first, mix_second], axis=1)
    block_count = TOKENS // TOK_DEV
    normed_blocks = normed.reshape(block_count, TOK_DEV, D).astype(jnp.float32)
    ids_blocks = expert_ids.reshape(block_count, TOK_DEV * 2)
    weight_blocks = mix_weight.reshape(block_count, TOK_DEV, 2)
    slot_range = jnp.arange(CAP, dtype=jnp.int32)
    first_in, second_in, first_out, second_out = expert_stack(u_gate_up, v_gate_up, u_down, v_down)

    def one_expert(carried, expert_index):
        member = (ids_blocks == expert_index).astype(jnp.int32)
        slot_of = jnp.cumsum(member, axis=1) - 1
        placed = (member[..., None] * (slot_of[..., None] == slot_range).astype(jnp.int32)).astype(jnp.float32)
        placed_tok = placed.reshape(block_count, TOK_DEV, 2, CAP)
        select = lax.optimization_barrier(jnp.sum(placed_tok, axis=2))
        rows_in = jnp.einsum('btc,btd->bcd', select, normed_blocks).astype(jnp.bfloat16)
        rows_in = rows_in.reshape(block_count * CAP, D)
        w_first = lax.dynamic_index_in_dim(first_in, expert_index, 0, keepdims=False)
        w_middle = lax.dynamic_index_in_dim(second_in, expert_index, 0, keepdims=False)
        w_down = lax.dynamic_index_in_dim(first_out, expert_index, 0, keepdims=False)
        w_last = lax.dynamic_index_in_dim(second_out, expert_index, 0, keepdims=False)
        rank_in = jnp.dot(rows_in, w_first, preferred_element_type=jnp.float32).astype(jnp.bfloat16)
        gate_part = jnp.dot(rank_in[:, :RANK], w_middle[0], preferred_element_type=jnp.float32)
        up_part = jnp.dot(rank_in[:, RANK:], w_middle[1], preferred_element_type=jnp.float32)
        hidden = (jax.nn.silu(gate_part) * up_part).astype(jnp.bfloat16)
        rank_down = jnp.dot(hidden, w_down, preferred_element_type=jnp.float32).astype(jnp.bfloat16)
        out_rows = jnp.dot(rank_down, w_last, preferred_element_type=jnp.float32).astype(jnp.bfloat16)
        back_rows = out_rows.astype(jnp.float32).reshape(block_count, CAP, D)
        weights_tok = jnp.einsum('btsc,bts->btc', placed_tok, weight_blocks)
        carried = carried + jnp.einsum('btc,bcd->btd', weights_tok, back_rows)
        return (carried, None)
    start_mix = jnp.zeros((block_count, TOK_DEV, D), jnp.float32)
    mixture, unused = lax.scan(one_expert, start_mix, jnp.arange(EXPERTS, dtype=jnp.int32))
    return (stream + mixture.reshape(TOKENS, D)).astype(jnp.bfloat16)
```

```python
import functools

import jax
import jax.numpy as jnp
from jax import lax
from jax.experimental import pallas as pl
from jax.experimental.pallas import tpu as pltpu
from jax.sharding import PartitionSpec as P

D = 6144
HEADS = 24
KV_HEADS = 4
HEAD_DIM = 128
EXPERTS = 8
RANK = 512
TOK_DEV = 128
CAP = 33


EPS = 1e-05
LOG2_E = 1.4426950408889634


def swapped(x, axis, distance):
    return lax.ppermute(x, axis, [(i, i ^ 1 << distance) for i in range(lax.axis_size(axis))])


def attention_kernel(heads, parts, q_ref, kv_ref, out_ref):
    block = pl.program_id(0)
    column = lax.axis_index("exp")
    columns = kv_ref.shape[0]
    span = columns // parts
    chunk = span * TOK_DEV
    rows = heads * TOK_DEV
    query = jnp.concatenate(
        [q_ref[:, h * HEAD_DIM : (h + 1) * HEAD_DIM] for h in range(heads)], axis=0
    )

    def step(index, carried, masked):
        row_max, row_sum, weighted = carried
        held = kv_ref[pl.ds((index % parts) * span, span), index // parts]
        held = held.reshape(chunk, 2 * HEAD_DIM)
        scores = lax.dot_general(
            query, held[:, :HEAD_DIM], (((1,), (1,)), ((), ())), preferred_element_type=jnp.float32
        ) * (HEAD_DIM ** (-0.5) * LOG2_E)
        if masked:
            offset = (column % span) * TOK_DEV
            own = lax.broadcasted_iota(jnp.int32, (rows, chunk), 0) % TOK_DEV + offset
            other = lax.broadcasted_iota(jnp.int32, (rows, chunk), 1)
            scores = jnp.where(other <= own, scores, -jnp.inf)
        new_max = jnp.maximum(row_max, jnp.max(scores, axis=-1, keepdims=True))
        fading = jnp.exp2(row_max - new_max)
        terms = jnp.exp2(scores - new_max)
        row_sum = row_sum * fading + jnp.sum(terms, axis=-1, keepdims=True)
        update = jnp.dot(
            terms.astype(jnp.bfloat16), held[:, HEAD_DIM:], preferred_element_type=jnp.float32
        )
        return new_max, row_sum, weighted * fading + update

    carried = (
        jnp.full((rows, 1), -1e30, jnp.float32),
        jnp.zeros((rows, 1), jnp.float32),
        jnp.zeros((rows, HEAD_DIM), jnp.float32),
    )
    last = block * parts + column // span
    carried = lax.fori_loop(0, last, lambda index, now: step(index, now, False), carried)
    row_max, row_sum, weighted = step(last, carried, True)
    result = (weighted / row_sum).astype(jnp.bfloat16)
    for h in range(heads):
        out_ref[:, h * HEAD_DIM : (h + 1) * HEAD_DIM] = result[h * TOK_DEV : (h + 1) * TOK_DEV]


def attention(query_rows, kv_all, heads):
    columns, blocks = kv_all.shape[:2]
    parts = max(1, columns * TOK_DEV // 512)
    width = heads * HEAD_DIM
    pairs = blocks * TOK_DEV * heads * columns * blocks * TOK_DEV // 2
    return pl.pallas_call(
        functools.partial(attention_kernel, heads, parts),
        grid=(blocks,),
        out_shape=jax.ShapeDtypeStruct((blocks * TOK_DEV, width), jnp.bfloat16),
        in_specs=[
            pl.BlockSpec((TOK_DEV, width), lambda b: (b, 0)),
            pl.BlockSpec(kv_all.shape, lambda b: (0, 0, 0, 0)),
        ],
        out_specs=pl.BlockSpec((TOK_DEV, width), lambda b: (b, 0)),
        compiler_params=pltpu.CompilerParams(vmem_limit_bytes=56 * 1024 * 1024),
        cost_estimate=pl.CostEstimate(
            flops=pairs * 4 * HEAD_DIM * 4,
            bytes_accessed=kv_all.size * 2,
            transcendentals=pairs,
        ),
        name="attention",
    )(query_rows, kv_all)


def middle_kernel(x_ref, v_ref, down_ref, out_ref, total):
    @pl.when(pl.program_id(0) == 0)
    def _():
        total[...] = jnp.zeros_like(total)

    gate = jnp.dot(x_ref[:, :RANK], v_ref[0, 0], preferred_element_type=jnp.float32)
    up = jnp.dot(x_ref[:, RANK:], v_ref[0, 1], preferred_element_type=jnp.float32)
    hidden = (gate / (1.0 + jnp.exp(-gate)) * up).astype(jnp.bfloat16)
    total[...] += jnp.dot(hidden, down_ref[0], preferred_element_type=jnp.float32)

    @pl.when(pl.program_id(0) == pl.num_programs(0) - 1)
    def _():
        out_ref[...] = total[...]


def middle(rank_in, v_gate_up, u_down):
    rows = rank_in.shape[0]
    units = u_down.shape[1]
    tile = min(1024, units)
    return pl.pallas_call(
        middle_kernel,
        grid=(units // tile,),
        out_shape=jax.ShapeDtypeStruct((rows, RANK), jnp.float32),
        in_specs=[
            pl.BlockSpec((rows, 2 * RANK), lambda i: (0, 0)),
            pl.BlockSpec((1, 2, RANK, tile), lambda i: (0, 0, 0, i)),
            pl.BlockSpec((1, tile, RANK), lambda i: (0, i, 0)),
        ],
        out_specs=pl.BlockSpec((rows, RANK), lambda i: (0, 0)),
        scratch_shapes=[pltpu.VMEM((rows, RANK), jnp.float32)],
        compiler_params=pltpu.CompilerParams(vmem_limit_bytes=48 * 1024 * 1024),
        cost_estimate=pl.CostEstimate(
            flops=rows * RANK * units * 6,
            bytes_accessed=units * RANK * 6,
            transcendentals=rows * units,
        ),
        name="middle",
    )(rank_in, v_gate_up, u_down)


def per_device(
    queries,
    keys,
    values,
    residual,
    proj_weight,
    norm_gain,
    router,
    expert_ids,
    u_gate_up,
    v_gate_up,
    u_down,
    v_down,
):
    seq_count = lax.axis_size("seq")
    exp_count = lax.axis_size("exp")
    heads = HEADS // seq_count
    shares = seq_count // KV_HEADS
    kv_send = jnp.concatenate(
        [keys.reshape(TOK_DEV, KV_HEADS, HEAD_DIM), values.reshape(TOK_DEV, KV_HEADS, HEAD_DIM)],
        axis=-1,
    )
    if shares > 1:
        kv_send = jnp.repeat(kv_send, shares, axis=1)
    kv_send = kv_send.reshape(TOK_DEV, seq_count * 2 * HEAD_DIM)
    kv_got = lax.all_to_all(kv_send, "seq", split_axis=1, concat_axis=0, tiled=True)
    kv_all = lax.all_gather(kv_got, "exp", axis=0, tiled=False)
    query_got = lax.all_to_all(queries, "seq", split_axis=1, concat_axis=0, tiled=True)
    query_got, weight_own = lax.optimization_barrier((query_got, proj_weight))
    weight_rows = lax.all_gather(weight_own, "seq", axis=0, tiled=True)
    kv_all = kv_all.reshape(exp_count, seq_count, TOK_DEV, 2 * HEAD_DIM)
    attended = attention(query_got, kv_all, heads)
    attended = lax.all_to_all(attended, "seq", split_axis=0, concat_axis=1, tiled=True)
    half = TOK_DEV // 2
    first_half, weight_rows = lax.optimization_barrier((attended[:half], weight_rows))
    gathered = [
        lax.all_gather(first_half, "exp", axis=0, tiled=True),
        lax.all_gather(attended[half:], "exp", axis=0, tiled=True),
    ]
    updates = []
    for rows in gathered:
        projected = jnp.dot(rows, weight_rows, preferred_element_type=jnp.float32)
        updates.append(
            lax.all_to_all(
                projected.astype(jnp.bfloat16), "exp", split_axis=0, concat_axis=1, tiled=True
            )
        )
    attn_update = jnp.concatenate(updates, axis=0)
    stream = residual.astype(jnp.float32) + attn_update.astype(jnp.float32)
    mean_sq = jnp.mean(stream * stream, axis=-1, keepdims=True)
    normed = (stream * lax.rsqrt(mean_sq + EPS) * norm_gain.astype(jnp.float32)).astype(
        jnp.bfloat16
    )
    logits = jnp.dot(normed, router, preferred_element_type=jnp.float32)
    expert_range = jnp.arange(EXPERTS, dtype=jnp.int32)
    picked = (expert_ids[:, :, None] == expert_range[None, None, :]).astype(jnp.float32)
    chosen = jnp.sum(picked * logits[:, None, :], axis=-1)
    mix_first = jax.nn.sigmoid(chosen[:, 0] - chosen[:, 1])
    mix_second = jax.nn.sigmoid(chosen[:, 1] - chosen[:, 0])
    piece_count = exp_count // EXPERTS
    piece_width = D // piece_count
    flat_ids = expert_ids.reshape(TOK_DEV * 2)
    member = (flat_ids[:, None] == expert_range[None, :]).astype(jnp.int32)
    slot_of = jnp.sum((jnp.cumsum(member, axis=0) - 1) * member, axis=1)
    dest = (flat_ids * CAP + slot_of).reshape(TOK_DEV, 2)
    places = jnp.arange(EXPERTS * CAP, dtype=jnp.int32)
    first_at = dest[:, 0:1] == places[None, :]
    second_at = dest[:, 1:2] == places[None, :]
    select = (first_at | second_at).astype(jnp.bfloat16)
    send_rows = lax.dot_general(
        select, normed, (((0,), (0,)), ((), ())), preferred_element_type=jnp.float32
    ).astype(jnp.bfloat16)
    if piece_count > 1:
        send_rows = send_rows.reshape(EXPERTS, CAP, piece_count, piece_width).transpose(0, 2, 1, 3)
    send_rows = send_rows.reshape(exp_count, CAP, piece_width)
    dispatched = lax.all_to_all(send_rows, "exp", split_axis=0, concat_axis=0, tiled=True)
    expert_rows = dispatched.reshape(exp_count * CAP, piece_width)
    rank_sum = jnp.dot(expert_rows, u_gate_up[0], preferred_element_type=jnp.float32)
    for bit_index in range(piece_count.bit_length() - 1):
        rank_sum = rank_sum + swapped(rank_sum.astype(jnp.bfloat16), "exp", bit_index).astype(
            rank_sum.dtype
        )
    down_sum = middle(rank_sum.astype(jnp.bfloat16), v_gate_up, u_down)
    for bit_index in range(piece_count.bit_length() - 1):
        down_sum = down_sum + swapped(down_sum.astype(jnp.bfloat16), "exp", bit_index).astype(
            down_sum.dtype
        )
    expert_out = jnp.dot(
        down_sum.astype(jnp.bfloat16), v_down[0], preferred_element_type=jnp.float32
    ).astype(jnp.bfloat16)
    returned = lax.all_to_all(
        expert_out.reshape(exp_count, CAP, piece_width),
        "exp",
        split_axis=0,
        concat_axis=0,
        tiled=True,
    )
    if piece_count > 1:
        returned = returned.reshape(EXPERTS, piece_count, CAP, piece_width).transpose(0, 2, 1, 3)
    returned_rows = returned.reshape(EXPERTS * CAP, D)
    mix = mix_first[:, None] * first_at.astype(jnp.float32) + mix_second[
        :, None
    ] * second_at.astype(jnp.float32)
    mix_high = lax.reduce_precision(mix, 8, 7)
    mix_low = (mix - mix_high).astype(jnp.bfloat16)
    mixture = jnp.dot(
        mix_high.astype(jnp.bfloat16), returned_rows, preferred_element_type=jnp.float32
    ) + jnp.dot(mix_low, returned_rows, preferred_element_type=jnp.float32)
    return (stream + mixture).astype(jnp.bfloat16)


def solution(mesh):
    in_specs = (
        P(("seq", "exp"), None),
        P(("seq", "exp"), None),
        P(("seq", "exp"), None),
        P(("seq", "exp"), None),
        P("seq", "exp"),
        P(),
        P(),
        P(("seq", "exp"), None),
        P("exp", None, None),
        P("exp", None, None, None),
        P("exp", None, None),
        P("exp", None, None),
    )
    out_specs = P(("seq", "exp"), None)
    return jax.shard_map(
        per_device, mesh=mesh, in_specs=in_specs, out_specs=out_specs, check_vma=False
    )
```
